32 devices in a mesh: space: 8 (over z, y), level: 4 (over x, core).
Axes of the slice: x: 2, y: 2, z: 4, core: 2. Of those that a mesh axis runs over, the one named last changes fastest.
Arguments:
- grid_latent: bfloat16 [4096, 512], P('space'), may hold values from -6 to 6
- mesh_latent: bfloat16 [4, 64, 512], P('level', 'space'), may hold values from -6 to 6
- grid_output_cotangent: bfloat16 [4096, 512], P('space'), may hold values from -6 to 6
- w_send: bfloat16 [512, 512], replicated, may hold values from -0.25 to 0.25
- w_recv: bfloat16 [512, 512], replicated, may hold values from -0.25 to 0.25
- output_weight: bfloat16 [512, 512], replicated, may hold values from -0.25 to 0.25
- hidden_layer_bias: float32 [512], replicated, may hold values from -4 to 4
- output_norm_gain: float32 [512], replicated, may hold values from 0.1 to 1.9
- edge_sender: int32 [4, 16384], P('level', 'space'), may hold values from 0 to 23
- edge_receiver: int32 [4, 16384], P('level', 'space'), may hold values from 0 to 511
- edge_live: int32 [4, 16384], P('level', 'space'), may hold values 0 or 1
Outputs:
- d_grid: float32 [4096, 512], P(('space', 'level'))
- d_mesh: float32 [4, 64, 512], P('level', 'space')
- d_w_send: bfloat16 [512, 512], replicated
- d_w_recv: bfloat16 [512, 512], replicated
- d_w_out: bfloat16 [512, 512], replicated
- d_bias: float32 [512], replicated
- d_gain: float32 [512], replicated
The draws below stay inside these ranges and needn't reach their ends.
All inputs are finite; a program needn't handle non-finite values. No bound on the sum of `edge_live` on one device may be relied on, other than what follows from the above.
Results may differ from the reference program's by a relative error of at most 0.012.
Values may be sent and summed in bfloat16 or wider, within the bound.
A program may use at most 64 MiB of HBM per device.

```python
import jax
import jax.numpy as jnp
from jax import lax

D = 512
G_DEV = 512
MESH_DEV = 8
LEVELS = 4
EDGE_SLOTS_SHARD = 2048
GRID = 4096
MESH_ROWS = 64
EDGES = 16384
N_SPACE = 8


def plant(result, stream_key, low, high):
    longest = result.shape.index(max(result.shape))
    spots = []
    for shift in (0, 1):
        where = [jax.random.randint(jax.random.fold_in(stream_key, axis), (), 0, length) for axis, length in enumerate(result.shape)]
        where[longest] = (where[longest] + shift) % result.shape[longest]
        spots.append(tuple(where))
    return result.at[spots[0]].set(low).at[spots[1]].set(high)


def block_levels(own_key, extent, pieces, least, top_value):
    def one(dim, blocks):
        heights = jax.random.uniform(jax.random.fold_in(jax.random.fold_in(own_key, 6), dim), (blocks,), jnp.float32, least / len(pieces), top_value / len(pieces))
        return jnp.repeat(jnp.exp(heights), extent[dim] // blocks).reshape((-1,) + (1,) * (len(extent) - dim - 1))

    loudness = one(*pieces[0])
    for cut in pieces[1:]:
        loudness = loudness * one(*cut)
    return loudness


def centred(own_key, extent, spread, bound, pieces=(), kind=jnp.bfloat16):
    result = spread * jax.random.normal(own_key, extent, jnp.float32)
    if pieces:
        result = result * block_levels(own_key, extent, pieces, -0.22, 0.18)
    return jnp.clip(result, -bound, bound).astype(kind)


def setup_inputs(seed: int = 0) -> dict:
    streams_of = jax.random.split(jax.random.key(seed), 12)
    return {
        "grid_latent": centred(streams_of[0], (GRID, D), 1.0, 6.0, ((0, 8),)),
        "mesh_latent": centred(streams_of[1], (LEVELS, MESH_ROWS, D), 1.0, 6.0, ((0, 4), (1, 8))),
        "grid_output_cotangent": centred(streams_of[2], (GRID, D), 1.0, 6.0, ((0, 8),)),
        "w_send": centred(streams_of[3], (D, D), D ** -0.5, 0.25),
        "w_recv": centred(streams_of[4], (D, D), D ** -0.5, 0.25),
        "output_weight": centred(streams_of[5], (D, D), D ** -0.5, 0.25),
        "hidden_layer_bias": centred(streams_of[6], (D,), 0.7, 4.0, (), jnp.float32),
        "output_norm_gain": jnp.clip(1.0 + 0.18 * jax.random.normal(streams_of[7], (D,), jnp.float32), 0.1, 1.9),
        "edge_sender": plant(jax.random.randint(streams_of[8], (LEVELS, EDGES), 0, 3 * MESH_DEV), jax.random.fold_in(streams_of[8], 1), 0, (3 * MESH_DEV) - 1).astype(jnp.int32),
        "edge_receiver": plant(jax.random.randint(streams_of[9], (LEVELS, EDGES), 0, G_DEV), jax.random.fold_in(streams_of[9], 1), 0, G_DEV - 1).astype(jnp.int32),
        "edge_live": plant((jax.random.randint(streams_of[10], (LEVELS, EDGES), 0, 4) < 3).astype(jnp.int32), jax.random.fold_in(streams_of[10], 1), 0, 1),
    }


def edge_reverse_step(sending_rows, receiver_rows, cotangent_lines, slot_active_flags, output_weight, hidden_layer_bias, output_norm_gain):
    preact = sending_rows + receiver_rows + hidden_layer_bias
    hidden = jax.nn.silu(preact).astype(jnp.bfloat16)
    outer = jnp.dot(hidden, output_weight, preferred_element_type=jnp.float32)
    center = outer - lax.optimization_barrier(jnp.mean(outer, axis=-1, keepdims=True))
    inv_scale = lax.rsqrt(lax.optimization_barrier(jnp.mean(center * center, axis=-1, keepdims=True)) + 1e-05)
    normed = center * inv_scale
    incoming_gradient = cotangent_lines.astype(jnp.float32) * slot_active_flags[:, None].astype(jnp.float32)
    scaled = incoming_gradient * output_norm_gain
    d_outer = inv_scale * (scaled - lax.optimization_barrier(jnp.mean(scaled, axis=-1, keepdims=True)) - normed * lax.optimization_barrier(jnp.mean(scaled * normed, axis=-1, keepdims=True)))
    d_outer_b = d_outer.astype(jnp.bfloat16)
    w_out_grad = jnp.dot(hidden.T, d_outer_b, preferred_element_type=jnp.float32)
    d_hidden = jnp.dot(d_outer_b, output_weight.T, preferred_element_type=jnp.float32)
    sigmoid = jax.nn.sigmoid(preact)
    preactivation_gradient = d_hidden * sigmoid * (1.0 + preact * (1.0 - sigmoid))
    return (preactivation_gradient, w_out_grad, lax.optimization_barrier(jnp.sum(preactivation_gradient, axis=0)), lax.optimization_barrier(jnp.sum(incoming_gradient * normed, axis=0)))

def reference(grid_latent, mesh_latent, grid_output_cotangent, w_send, w_recv, output_weight, hidden_layer_bias, output_norm_gain, edge_sender, edge_receiver, edge_live):
    proj_send = jnp.einsum('lmd,de->lme', mesh_latent.astype(jnp.float32), w_send.astype(jnp.float32)).astype(jnp.bfloat16)
    projected_receiver = jnp.dot(grid_latent, w_recv, preferred_element_type=jnp.float32)
    mesh_levels = []
    grid_total = jnp.zeros((GRID, D), jnp.float32)
    wout_acc = jnp.zeros((D, D), jnp.float32)
    bias_acc = jnp.zeros((D,), jnp.float32)
    gain_acc = jnp.zeros((D,), jnp.float32)
    for level in range(LEVELS):
        level_table = proj_send[level]
        senders = edge_sender[level]
        receivers = edge_receiver[level]
        active_slots = edge_live[level]

        def visit(carry, shard):
            mesh_acc, grid_acc, wout_sum, bias_sum, gain_sum = carry
            start_offset = (shard * EDGE_SLOTS_SHARD).astype(jnp.int32)
            sender_local = lax.dynamic_slice_in_dim(senders, start_offset, EDGE_SLOTS_SHARD)
            recv_local = lax.dynamic_slice_in_dim(receivers, start_offset, EDGE_SLOTS_SHARD)
            slot_active_flags = lax.dynamic_slice_in_dim(active_slots, start_offset, EDGE_SLOTS_SHARD)
            target = shard + sender_local // MESH_DEV - 1
            target = jnp.where((target < 0) | (target >= N_SPACE), shard, target).astype(jnp.int32)
            global_row = (target * MESH_DEV + sender_local % MESH_DEV).astype(jnp.int32)
            receiver_index = (recv_local + shard * G_DEV).astype(jnp.int32)
            sending_rows = level_table[global_row].astype(jnp.float32)
            preactivation_gradient, output_weight_piece, bias_piece, gain_piece = edge_reverse_step(sending_rows, projected_receiver[receiver_index], grid_output_cotangent[receiver_index], slot_active_flags, output_weight, hidden_layer_bias, output_norm_gain)
            mesh_acc = mesh_acc.at[global_row].add(preactivation_gradient)
            grid_acc = grid_acc.at[receiver_index].add(preactivation_gradient)
            return ((mesh_acc, grid_acc, wout_sum + output_weight_piece, bias_sum + bias_piece, gain_sum + gain_piece), None)
        start_carry = (jnp.zeros((MESH_ROWS, D), jnp.float32), jnp.zeros((GRID, D), jnp.float32), wout_acc, bias_acc, gain_acc)
        final, _ = lax.scan(visit, start_carry, jnp.arange(N_SPACE, dtype=jnp.int32))
        mesh_level, grid_level, wout_acc, bias_acc, gain_acc = final
        mesh_levels.append(mesh_level)
        grid_total = grid_total + grid_level.astype(jnp.bfloat16).astype(jnp.float32)
    mesh_sum = jnp.stack(mesh_levels, axis=0).astype(jnp.bfloat16)
    grid_sum = grid_total.astype(jnp.bfloat16)
    d_mesh = jnp.einsum('lmd,ed->lme', mesh_sum.astype(jnp.float32), w_send.astype(jnp.float32))
    d_grid = jnp.dot(grid_sum, w_recv.T, preferred_element_type=jnp.float32)
    d_w_send = jnp.einsum('lmd,lme->de', mesh_latent.astype(jnp.float32), mesh_sum.astype(jnp.float32))
    d_w_recv = jnp.dot(grid_latent.T, grid_sum, preferred_element_type=jnp.float32)
    return (d_grid, d_mesh, d_w_send.astype(jnp.bfloat16), d_w_recv.astype(jnp.bfloat16), wout_acc.astype(jnp.bfloat16), bias_acc, gain_acc)
```

```python
import functools

import jax
import jax.numpy as jnp
from jax import lax
from jax.experimental import pallas as pl
from jax.experimental.pallas import tpu as pltpu
from jax.sharding import PartitionSpec as P

MESH = pl.DeviceIdType.MESH
F32 = jnp.float32
BF16 = jnp.bfloat16
TILE = 16


def mm(a, b, ca=1, cb=0):
    return lax.dot_general(a, b, (((ca,), (cb,)), ((), ())), preferred_element_type=F32)


def bit_steps(axis, count):
    steps = []
    width = 1
    while width < count:
        steps.append((axis, width))
        width *= 2
    return steps


def partner(axis, width):
    me = lax.axis_index(axis)
    bit = (me // width) % 2
    return bit, {axis: me + (1 - 2 * bit) * width}


def halvings(rows, steps):
    plan = []
    size = rows
    for axis, width in steps:
        split = (size // 2) % TILE == 0
        plan.append((axis, width, size, split))
        if split:
            size //= 2
    return plan, size


def reversed_chunks(count):
    order = [0]
    width = 1
    while width < count:
        order = [2 * c for c in order] + [2 * c + 1 for c in order]
        width *= 2
    return order


def kernel(
    n_space,
    n_level,
    block,
    grid_ref,
    mesh_ref,
    cot_ref,
    wsend_ref,
    wrecv_ref,
    wout_ref,
    bias_ref,
    gain_ref,
    snd_ref,
    rcv_ref,
    live_ref,
    dgrid_ref,
    dmesh_ref,
    dw_ref,
    dvec_ref,
    window,
    table,
    proj,
    wacc,
    gacc,
    macc,
    vacc,
    red,
    red_in,
    gbuf,
    gbuf_in,
    vec,
    vec_in,
    mout,
    m_in,
    halo_sem,
    mgrad_sem,
    red_sem,
    gat_sem,
    grid_sem,
    vec_sem,
):
    rows, width = grid_ref.shape
    mrows = mesh_ref.shape[0]
    slots = snd_ref.shape[1]
    band = lax.axis_index("space")
    steps = bit_steps("level", n_level) + bit_steps("space", n_space)
    first = band > 0
    last = band < n_space - 1
    pad = table.shape[0]

    window[...] = jnp.zeros_like(window)
    macc[...] = jnp.zeros_like(macc)
    m_in[...] = jnp.zeros_like(m_in)
    barrier = pltpu.get_barrier_semaphore()
    for axis, w in steps:
        _, who = partner(axis, w)
        pl.semaphore_signal(barrier, inc=1, device_id=who, device_id_type=MESH)
    up = {"space": (band + 1) % n_space}
    down = {"space": (band + n_space - 1) % n_space}
    pl.semaphore_signal(barrier, inc=1, device_id=up, device_id_type=MESH)
    pl.semaphore_signal(barrier, inc=1, device_id=down, device_id_type=MESH)
    pl.semaphore_wait(barrier, len(steps) + 2)

    def remote(src, dst, sem, who):
        return pltpu.make_async_remote_copy(
            src_ref=src,
            dst_ref=dst,
            send_sem=sem.at[0],
            recv_sem=sem.at[1],
            device_id=who,
            device_id_type=MESH,
        )

    to_up = remote(mesh_ref, window.at[0], halo_sem.at[0], up)
    to_down = remote(mesh_ref, window.at[2], halo_sem.at[1], down)

    @pl.when(last)
    def _():
        to_up.start()

    @pl.when(first)
    def _():
        to_down.start()

    window[1] = mesh_ref[...]
    proj[...] = mm(grid_ref[...], wrecv_ref[...]).astype(BF16)
    wacc[...] = jnp.zeros_like(wacc)
    gacc[...] = jnp.zeros_like(gacc)
    vacc[...] = jnp.zeros_like(vacc)

    @pl.when(last)
    def _():
        to_up.wait_send()
        to_down.wait_recv()

    @pl.when(first)
    def _():
        to_down.wait_send()
        to_up.wait_recv()

    win = jnp.concatenate(
        [window[k].astype(F32) for k in range(3)] + [jnp.zeros((pad - 3 * mrows, width), F32)], axis=0
    ).astype(BF16)
    table[...] = mm(win, wsend_ref[...]).astype(BF16)

    def step(i, _):
        at = pl.ds(pl.multiple_of(i * block, block), block)
        snd = snd_ref[:, at]
        rcv = rcv_ref[:, at]
        live = live_ref[:, at]
        slot = snd // mrows
        target = band + slot - 1
        slot = jnp.where((target >= 0) & (target < n_space), slot, 1)
        src = slot * mrows + snd % mrows

        def column(v):
            return jnp.transpose(jnp.broadcast_to(v, (128, block)))

        rcv_c = column(rcv)
        src_c = column(src)
        live_c = column(live.astype(F32))
        reps = rows // 128
        wreps = width // 128
        pick = (
            jnp.concatenate([rcv_c] * reps, axis=1)
            == lax.broadcasted_iota(jnp.int32, (block, rows), 1)
        ).astype(F32).astype(BF16)
        pick_s = (
            jnp.concatenate([src_c] * (pad // 128), axis=1)
            == lax.broadcasted_iota(jnp.int32, (block, pad), 1)
        ).astype(F32).astype(BF16)
        put = (
            jnp.broadcast_to(rcv, (rows, block))
            == lax.broadcasted_iota(jnp.int32, (rows, block), 0)
        ).astype(F32).astype(BF16)
        put_s = (
            jnp.broadcast_to(src, (macc.shape[0], block))
            == lax.broadcasted_iota(jnp.int32, (macc.shape[0], block), 0)
        ).astype(F32).astype(BF16)

        preact = mm(pick, proj[...]) + mm(pick_s, table[...]) + bias_ref[...]
        sig = jax.nn.sigmoid(preact)
        hidden = (preact * sig).astype(BF16)
        outer = mm(hidden, wout_ref[...])
        center = outer - jnp.mean(outer, axis=-1, keepdims=True)
        inv = lax.rsqrt(jnp.mean(center * center, axis=-1, keepdims=True) + 1e-05)
        normed = center * inv
        upstream = mm(pick, cot_ref[...]) * jnp.concatenate([live_c] * wreps, axis=1)
        scaled = upstream * gain_ref[...]
        d_outer = inv * (
            scaled
            - jnp.mean(scaled, axis=-1, keepdims=True)
            - normed * jnp.mean(scaled * normed, axis=-1, keepdims=True)
        )
        d_outer = d_outer.astype(BF16)
        wacc[...] += mm(hidden, d_outer, 0, 0)
        d_pre = mm(d_outer, wout_ref[...], 1, 1) * (sig * (1.0 + preact * (1.0 - sig)))
        vacc[0] += jnp.sum(d_pre.reshape(block // 8, 8, width), axis=0)
        vacc[1] += jnp.sum((upstream * normed).reshape(block // 8, 8, width), axis=0)
        d_pre = d_pre.astype(BF16)
        gacc[...] += mm(put, d_pre)
        macc[...] += mm(put_s, d_pre)
        return 0

    lax.fori_loop(0, slots // block, step, 0)

    mout[0] = macc[0:mrows]
    mout[1] = macc[2 * mrows : 3 * mrows]
    g_up = remote(mout.at[1], m_in.at[0], mgrad_sem.at[0], up)
    g_down = remote(mout.at[0], m_in.at[1], mgrad_sem.at[1], down)

    @pl.when(last)
    def _():
        g_up.start()

    @pl.when(first)
    def _():
        g_down.start()

    vec[0] = jnp.concatenate(
        [jnp.sum(vacc[k], axis=0, keepdims=True) for k in range(2)], axis=0
    )
    share = rows // n_level
    for place, chunk in enumerate(reversed_chunks(n_level)):
        gbuf[place * share : (place + 1) * share] = gacc[chunk * share : (chunk + 1) * share].astype(BF16)
    red[0:width] = wacc[...].astype(BF16)
    red[width : 2 * width] = mm(grid_ref[...], gacc[...].astype(BF16), 0, 0).astype(BF16)
    red[2 * width : 3 * width] = mm(win, jnp.concatenate(
        [macc[0 : 3 * mrows], jnp.zeros((pad - 3 * mrows, width), F32)], axis=0
    ).astype(BF16), 0, 0).astype(BF16)

    plan, _ = halvings(red.shape[0], steps)
    off = 0
    goff = 0
    gsize = rows
    spot = 0
    trail = []
    for k, (axis, w, size, split) in enumerate(plan):
        bit, who = partner(axis, w)
        half = size // 2 if split else size
        give = off + (1 - bit) * half if split else off
        keep = off + bit * half if split else off
        at_give = pl.ds(pl.multiple_of(give, TILE), half)
        at_keep = pl.ds(pl.multiple_of(keep, TILE), half)
        into = red_in.at[pl.ds(spot, half)]
        copies = [
            remote(red.at[at_give], into, red_sem.at[k], who),
            remote(vec.at[k], vec_in.at[k], vec_sem.at[k], who),
        ]
        if axis == "level":
            gsize //= 2
            g_give = pl.ds(pl.multiple_of(goff + (1 - bit) * gsize, TILE), gsize)
            g_keep = pl.ds(pl.multiple_of(goff + bit * gsize, TILE), gsize)
            g_into = gbuf_in.at[pl.ds(rows - 2 * gsize, gsize)]
            copies.append(remote(gbuf.at[g_give], g_into, grid_sem.at[k], who))
            goff = goff + bit * gsize
        for c in copies:
            c.start()
        for c in copies:
            c.wait()
        red[at_keep] = (red[at_keep].astype(F32) + red_in[pl.ds(spot, half)].astype(F32)).astype(BF16)
        vec[k + 1] = vec[k] + vec_in[k]
        if axis == "level":
            gbuf[g_keep] = (
                gbuf[g_keep].astype(F32) + gbuf_in[pl.ds(rows - 2 * gsize, gsize)].astype(F32)
            ).astype(BF16)
        spot += half
        if split:
            trail.append((k, who, half))
        off = keep
    dvec_ref[...] = vec[len(plan)]

    held = trail[-1][2]
    at = pl.ds(pl.multiple_of(off, TILE), held)
    dw_ref[at] = red[at]
    for k, who, half in reversed(trail):
        at = pl.ds(pl.multiple_of(off, TILE), half)
        c = remote(dw_ref.at[at], dw_ref.at[at], gat_sem.at[k], who)
        c.start()
        if k == trail[-1][0]:
            g_at = pl.ds(pl.multiple_of(goff, TILE), share)
            dgrid_ref[...] = mm(gbuf[g_at], wrecv_ref[...], 1, 1)

            @pl.when(last)
            def _():
                g_up.wait_send()
                g_down.wait_recv()

            @pl.when(first)
            def _():
                g_down.wait_send()
                g_up.wait_recv()

            total = macc[mrows : 2 * mrows] + m_in[0] + m_in[1]
            total = jnp.concatenate([total, jnp.zeros((TILE - mrows % TILE, width), F32)], axis=0)
            dmesh_ref[...] = mm(total.astype(BF16), wsend_ref[...], 1, 1)[0:mrows]
        c.wait()
        off = off - ((off // half) % 2) * half


def body(
    grid_latent,
    mesh_latent,
    grid_output_cotangent,
    w_send,
    w_recv,
    output_weight,
    hidden_layer_bias,
    output_norm_gain,
    edge_sender,
    edge_receiver,
    edge_live,
):
    n_space = lax.axis_size("space")
    n_level = lax.axis_size("level")
    rows, width = grid_latent.shape
    mrows = mesh_latent.shape[1]
    slots = edge_sender.shape[1]
    block = min(256, slots)
    pad = -(-3 * mrows // 128) * 128
    mpad = -(-3 * mrows // TILE) * TILE
    steps = bit_steps("level", n_level) + bit_steps("space", n_space)
    n = len(steps)
    plan, _ = halvings(3 * width, steps)
    inbox = sum(size // 2 if split else size for _, _, size, split in plan)
    vm = pl.BlockSpec(memory_space=pltpu.VMEM)
    dma = pltpu.SemaphoreType.DMA
    d_grid, d_mesh, d_w, d_vec = pl.pallas_call(
        functools.partial(kernel, n_space, n_level, block),
        out_shape=(
            jax.ShapeDtypeStruct((rows // n_level, width), F32),
            jax.ShapeDtypeStruct((mrows, width), F32),
            jax.ShapeDtypeStruct((3 * width, width), BF16),
            jax.ShapeDtypeStruct((2, width), F32),
        ),
        in_specs=[vm] * 11,
        out_specs=(vm,) * 4,
        scratch_shapes=[
            pltpu.VMEM((3, mrows, width), BF16),
            pltpu.VMEM((pad, width), BF16),
            pltpu.VMEM((rows, width), BF16),
            pltpu.VMEM((width, width), F32),
            pltpu.VMEM((rows, width), F32),
            pltpu.VMEM((mpad, width), F32),
            pltpu.VMEM((2, 8, width), F32),
            pltpu.VMEM((3 * width, width), BF16),
            pltpu.VMEM((inbox, width), BF16),
            pltpu.VMEM((rows, width), BF16),
            pltpu.VMEM((rows, width), BF16),
            pltpu.VMEM((n + 1, 2, width), F32),
            pltpu.VMEM((n, 2, width), F32),
            pltpu.VMEM((2, mrows, width), F32),
            pltpu.VMEM((2, mrows, width), F32),
            dma((2, 2)),
            dma((2, 2)),
            dma((n, 2)),
            dma((n, 2)),
            dma((n, 2)),
            dma((n, 2)),
        ],
        compiler_params=pltpu.CompilerParams(collective_id=0, has_side_effects=True),
        name="edge_backward",
    )(
        grid_latent,
        mesh_latent[0],
        grid_output_cotangent,
        w_send,
        w_recv,
        output_weight,
        hidden_layer_bias[None],
        output_norm_gain[None],
        edge_sender,
        edge_receiver,
        edge_live,
    )
    return (
        d_grid,
        d_mesh[None],
        d_w[2 * width :],
        d_w[width : 2 * width],
        d_w[:width],
        d_vec[0],
        d_vec[1],
    )


def solution(mesh):
    return jax.shard_map(
        body,
        mesh=mesh,
        in_specs=(
            P("space", None),
            P("level", "space", None),
            P("space", None),
            P(),
            P(),
            P(),
            P(),
            P(),
            P("level", "space"),
            P("level", "space"),
            P("level", "space"),
        ),
        out_specs=(P(("space", "level"), None), P("level", "space", None), P(), P(), P(), P(), P()),
        check_vma=False,
    )
```

```python
import functools

import jax
import jax.numpy as jnp
from jax import lax
from jax.experimental import pallas as pl
from jax.experimental.pallas import tpu as pltpu
from jax.sharding import PartitionSpec as P

MESH = pl.DeviceIdType.MESH
F32 = jnp.float32
BF16 = jnp.bfloat16
TILE = 16


def mm(a, b, ca=1, cb=0):
    return lax.dot_general(a, b, (((ca,), (cb,)), ((), ())), preferred_element_type=F32)


def bit_steps(axis, count):
    steps = []
    width = 1
    while width < count:
        steps.append((axis, width))
        width *= 2
    return steps


def partner(axis, width):
    me = lax.axis_index(axis)
    bit = (me // width) % 2
    return bit, {axis: me + (1 - 2 * bit) * width}


def reversed_chunks(count):
    order = [0]
    width = 1
    while width < count:
        order = [2 * c for c in order] + [2 * c + 1 for c in order]
        width *= 2
    return order


def step_orders(n_space, n_level):
    level = bit_steps("level", n_level)
    space = bit_steps("space", n_space)
    return level + space, level[:-1] + space[:1] + level[-1:] + space[1:]


def halvings(rows, steps):
    plan = []
    size = rows
    for axis, width in steps:
        split = (size // 2) % TILE == 0
        plan.append((axis, width, size, split))
        if split:
            size //= 2
    return plan


def inbox_rows(rows, steps):
    return sum(size // 2 if split else size for _, _, size, split in halvings(rows, steps))


def remote(src, dst, sem, who):
    return pltpu.make_async_remote_copy(
        src_ref=src,
        dst_ref=dst,
        send_sem=sem.at[0],
        recv_sem=sem.at[1],
        device_id=who,
        device_id_type=MESH,
    )


def reduce_lane(buf, out, inbox, cols, sem_r, sem_g, steps):
    off = 0
    spot = 0
    trail = []
    for k, (axis, w, size, split) in enumerate(halvings(buf.shape[0], steps)):
        bit, who = partner(axis, w)
        half = size // 2 if split else size
        give = off + (1 - bit) * half if split else off
        keep = off + bit * half if split else off
        at_give = pl.ds(pl.multiple_of(give, TILE), half)
        at_keep = pl.ds(pl.multiple_of(keep, TILE), half)
        into = pl.ds(spot, half)
        c = remote(buf.at[at_give, cols], inbox.at[into], sem_r.at[k], who)
        c.start()
        yield
        c.wait()
        buf[at_keep, cols] = (buf[at_keep, cols].astype(F32) + inbox[into].astype(F32)).astype(BF16)
        spot += half
        off = keep
        if split:
            trail.append((k, who, half, bit))
    at = pl.ds(pl.multiple_of(off, TILE), trail[-1][2])
    out[at, cols] = buf[at, cols]
    for k, who, half, bit in reversed(trail):
        at = pl.ds(pl.multiple_of(off, TILE), half)
        c = remote(out.at[at, cols], out.at[at, cols], sem_g.at[k], who)
        c.start()
        yield
        c.wait()
        off = off - bit * half


def gather_lane(buf, sem, steps):
    base = gather_place(steps)
    for j, (axis, w) in enumerate(reversed(steps)):
        bit, who = partner(axis, w)
        at = pl.ds(base, 1 << j)
        c = remote(buf.at[at], buf.at[at], sem.at[j], who)
        c.start()
        yield
        c.wait()
        base = base - bit * (1 << j)


def gather_place(steps):
    place = 0
    for j, (axis, w) in enumerate(reversed(steps)):
        place = place + partner(axis, w)[0] * (1 << j)
    return place


def grid_lane(gbuf, inbox, dgrid_ref, wrecv_ref, sem, n_level):
    off = 0
    size = gbuf.shape[0]
    spot = 0
    for k, (axis, w) in enumerate(bit_steps("level", n_level)):
        bit, who = partner(axis, w)
        size //= 2
        give = pl.ds(pl.multiple_of(off + (1 - bit) * size, TILE), size)
        keep = pl.ds(pl.multiple_of(off + bit * size, TILE), size)
        into = pl.ds(spot, size)
        c = remote(gbuf.at[give], inbox.at[into], sem.at[k], who)
        c.start()
        yield
        c.wait()
        gbuf[keep] = (gbuf[keep].astype(F32) + inbox[into].astype(F32)).astype(BF16)
        spot += size
        off = off + bit * size
    dgrid_ref[...] = mm(gbuf[pl.ds(pl.multiple_of(off, TILE), size)], wrecv_ref[...], 1, 1)


def vec_lane(vec, inbox, dvec_ref, sem, steps):
    for k, (axis, w) in enumerate(steps):
        _, who = partner(axis, w)
        c = remote(vec.at[k], inbox.at[k], sem.at[k], who)
        c.start()
        yield
        c.wait()
        vec[k + 1] = vec[k] + inbox[k]
    dvec_ref[...] = vec[len(steps)]


def edge_copies(up, down):
    n_space = lax.axis_size("space")
    band = lax.axis_index("space")
    first = band > 0
    last = band < n_space - 1

    def start():
        @pl.when(last)
        def _():
            up.start()

        @pl.when(first)
        def _():
            down.start()

    def wait():
        @pl.when(last)
        def _():
            up.wait_send()
            down.wait_recv()

        @pl.when(first)
        def _():
            down.wait_send()
            up.wait_recv()

    return start, wait


def advance(lanes):
    for lane in list(lanes):
        if next(lane, "end") == "end":
            lanes.remove(lane)


def kernel(
    n_space,
    n_level,
    block,
    segments,
    grid_ref,
    mesh_ref,
    cot_ref,
    wsend_ref,
    wrecv_ref,
    wout_ref,
    bias_ref,
    gain_ref,
    snd_ref,
    rcv_ref,
    live_ref,
    dgrid_ref,
    dmesh_ref,
    dwo_ref,
    dwr_ref,
    dws_ref,
    dvec_ref,
    window,
    table,
    proj,
    pre,
    ups,
    dout,
    wacc,
    gacc,
    macc,
    vacc,
    red_o,
    red_r,
    inbox,
    gbuf,
    gbuf_in,
    vec,
    vec_in,
    mout,
    m_in,
    mesh_all,
    sum_all,
    halo_sem,
    mgrad_sem,
    red_sem,
    gat_sem,
    mesh_sem,
    grid_sem,
    vec_sem,
):
    rows, width = grid_ref.shape
    mrows = mesh_ref.shape[0]
    slots = snd_ref.shape[1]
    band = lax.axis_index("space")
    steps, swapped = step_orders(n_space, n_level)
    pad = table.shape[0]

    window[...] = jnp.zeros_like(window)
    m_in[...] = jnp.zeros_like(m_in)
    barrier = pltpu.get_barrier_semaphore()
    for axis, w in steps:
        _, who = partner(axis, w)
        pl.semaphore_signal(barrier, inc=1, device_id=who, device_id_type=MESH)
    up = {"space": (band + 1) % n_space}
    down = {"space": (band + n_space - 1) % n_space}
    pl.semaphore_signal(barrier, inc=1, device_id=up, device_id_type=MESH)
    pl.semaphore_signal(barrier, inc=1, device_id=down, device_id_type=MESH)
    macc[...] = jnp.zeros_like(macc)
    wacc[...] = jnp.zeros_like(wacc)
    gacc[...] = jnp.zeros_like(gacc)
    vacc[...] = jnp.zeros_like(vacc)
    window[1] = mesh_ref[...]
    place = gather_place(steps)
    mesh_all[place] = mesh_ref[...]
    proj[...] = mm(grid_ref[...], wrecv_ref[...]).astype(BF16)
    pl.semaphore_wait(barrier, len(steps) + 2)

    halo_start, halo_wait = edge_copies(
        remote(mesh_ref, window.at[0], halo_sem.at[0], up),
        remote(mesh_ref, window.at[2], halo_sem.at[1], down),
    )
    halo_start()
    early = [gather_lane(mesh_all, mesh_sem.at[0], steps)]
    advance(early)

    def span(i):
        return pl.ds(pl.multiple_of(i * block, block), block)

    def column(v):
        return jnp.transpose(jnp.broadcast_to(v, (128, block)))

    def one_hot(hit):
        return hit.astype(F32).astype(BF16)

    def source(at):
        snd = snd_ref[:, at]
        slot = snd // mrows
        target = band + slot - 1
        slot = jnp.where((target >= 0) & (target < n_space), slot, 1)
        return slot * mrows + snd % mrows

    def gathers(i, _):
        at = span(i)
        rcv_c = column(rcv_ref[:, at])
        live_c = column(live_ref[:, at].astype(F32))
        pick = one_hot(
            jnp.concatenate([rcv_c] * (rows // 128), axis=1)
            == lax.broadcasted_iota(jnp.int32, (block, rows), 1)
        )
        pre[at] = mm(pick, proj[...]) + bias_ref[...]
        ups[at] = (mm(pick, cot_ref[...]) * jnp.concatenate([live_c] * (width // 128), axis=1)).astype(BF16)
        return 0

    count = slots // block
    lax.fori_loop(0, count, gathers, 0)

    halo_wait()
    win = jnp.concatenate(
        [window[k].astype(F32) for k in range(3)] + [jnp.zeros((pad - 3 * mrows, width), F32)], axis=0
    ).astype(BF16)
    table[...] = mm(win, wsend_ref[...]).astype(BF16)

    def forward(i, _):
        at = span(i)
        src_c = column(source(at))
        pick = one_hot(
            jnp.concatenate([src_c] * (pad // 128), axis=1)
            == lax.broadcasted_iota(jnp.int32, (block, pad), 1)
        )
        preact = pre[at] + mm(pick, table[...])
        sig = jax.nn.sigmoid(preact)
        hidden = (preact * sig).astype(BF16)
        pre[at] = sig * (1.0 + preact * (1.0 - sig))
        outer = mm(hidden, wout_ref[...])
        center = outer - jnp.mean(outer, axis=-1, keepdims=True)
        inv = lax.rsqrt(jnp.mean(center * center, axis=-1, keepdims=True) + 1e-05)
        normed = center * inv
        upstream = ups[at].astype(F32)
        scaled = upstream * gain_ref[...]
        d_outer = inv * (
            scaled
            - jnp.mean(scaled, axis=-1, keepdims=True)
            - normed * jnp.mean(scaled * normed, axis=-1, keepdims=True)
        )
        d_outer = d_outer.astype(BF16)
        dout[at] = d_outer
        wacc[...] += mm(hidden, d_outer, 0, 0)
        vacc[1] += jnp.sum((upstream * normed).reshape(block // 8, 8, width), axis=0)
        return 0

    def backward(i, _):
        at = span(i)
        put = one_hot(
            jnp.broadcast_to(rcv_ref[:, at], (rows, block))
            == lax.broadcasted_iota(jnp.int32, (rows, block), 0)
        )
        put_s = one_hot(
            jnp.broadcast_to(source(at), (macc.shape[0], block))
            == lax.broadcasted_iota(jnp.int32, (macc.shape[0], block), 0)
        )
        d_pre = mm(dout[at], wout_ref[...], 1, 1) * pre[at]
        vacc[0] += jnp.sum(d_pre.reshape(block // 8, 8, width), axis=0)
        d_pre = d_pre.astype(BF16)
        gacc[...] += mm(put, d_pre)
        macc[...] += mm(put_s, d_pre)
        return 0

    cuts = [count * k // segments for k in range(segments + 1)]
    for lo, hi in zip(cuts, cuts[1:]):
        lax.fori_loop(lo, hi, forward, 0)
        advance(early)

    half = width // 2
    sides = [(pl.ds(0, half), steps), (pl.ds(half, half), swapped)]

    def reducers(buf, out, at):
        return [
            reduce_lane(buf, out, inbox.at[at + k], cols, red_sem.at[at + k], gat_sem.at[at + k], order)
            for k, (cols, order) in enumerate(sides)
        ]

    red_o[...] = wacc[...].astype(BF16)
    out_lanes = reducers(red_o, dwo_ref, 0) + early
    advance(out_lanes)
    for lo, hi in zip(cuts, cuts[1:]):
        lax.fori_loop(lo, hi, backward, 0)
        if hi < count:
            advance(out_lanes)

    red_r[...] = mm(grid_ref[...], gacc[...].astype(BF16), 0, 0).astype(BF16)
    lanes = reducers(red_r, dwr_ref, 2)
    advance(lanes)

    def mesh_lane():
        mout[0] = macc[0:mrows]
        mout[1] = macc[2 * mrows : 3 * mrows]
        start, wait = edge_copies(
            remote(mout.at[1], m_in.at[0], mgrad_sem.at[0], up),
            remote(mout.at[0], m_in.at[1], mgrad_sem.at[1], down),
        )
        start()
        yield
        wait()
        total = macc[mrows : 2 * mrows] + m_in[0] + m_in[1]
        sum_all[place] = total.astype(BF16)
        lane = gather_lane(sum_all, mesh_sem.at[1], steps)
        next(lane)
        total = jnp.concatenate([total, jnp.zeros((TILE - mrows % TILE, width), F32)], axis=0)
        dmesh_ref[...] = mm(total.astype(BF16), wsend_ref[...], 1, 1)[0:mrows]
        yield
        yield from lane
        every = mesh_all.shape[0] * mrows
        dws_ref[...] = mm(
            mesh_all[...].astype(F32).reshape(every, width).astype(BF16),
            sum_all[...].astype(F32).reshape(every, width).astype(BF16),
            0,
            0,
        ).astype(BF16)

    share = rows // n_level
    for spot, chunk in enumerate(reversed_chunks(n_level)):
        gbuf[spot * share : (spot + 1) * share] = gacc[chunk * share : (chunk + 1) * share].astype(BF16)
    vec[0] = jnp.concatenate([jnp.sum(vacc[k], axis=0, keepdims=True) for k in range(2)], axis=0)
    small = [
        mesh_lane(),
        grid_lane(gbuf, gbuf_in, dgrid_ref, wrecv_ref, grid_sem, n_level),
        vec_lane(vec, vec_in, dvec_ref, vec_sem, steps),
    ]
    advance(small)
    lanes = lanes + small + out_lanes
    while lanes:
        advance(lanes)


def body(
    grid_latent,
    mesh_latent,
    grid_output_cotangent,
    w_send,
    w_recv,
    output_weight,
    hidden_layer_bias,
    output_norm_gain,
    edge_sender,
    edge_receiver,
    edge_live,
):
    n_space = lax.axis_size("space")
    n_level = lax.axis_size("level")
    rows, width = grid_latent.shape
    mrows = mesh_latent.shape[1]
    slots = edge_sender.shape[1]
    block = min(256, slots)
    pad = -(-3 * mrows // 128) * 128
    mpad = -(-3 * mrows // TILE) * TILE
    steps = bit_steps("level", n_level) + bit_steps("space", n_space)
    n = len(steps)
    inbox = inbox_rows(width, steps)
    vm = pl.BlockSpec(memory_space=pltpu.VMEM)
    dma = pltpu.SemaphoreType.DMA
    everyone = n_space * n_level
    d_grid, d_mesh, d_w_out, d_w_recv, d_w_send, d_vec = pl.pallas_call(
        functools.partial(kernel, n_space, n_level, block, min(4, slots // block)),
        out_shape=(
            jax.ShapeDtypeStruct((rows // n_level, width), F32),
            jax.ShapeDtypeStruct((mrows, width), F32),
            jax.ShapeDtypeStruct((width, width), BF16),
            jax.ShapeDtypeStruct((width, width), BF16),
            jax.ShapeDtypeStruct((width, width), BF16),
            jax.ShapeDtypeStruct((2, width), F32),
        ),
        in_specs=[vm] * 11,
        out_specs=(vm,) * 6,
        scratch_shapes=[
            pltpu.VMEM((3, mrows, width), BF16),
            pltpu.VMEM((pad, width), BF16),
            pltpu.VMEM((rows, width), BF16),
            pltpu.VMEM((slots, width), F32),
            pltpu.VMEM((slots, width), BF16),
            pltpu.VMEM((slots, width), BF16),
            pltpu.VMEM((width, width), F32),
            pltpu.VMEM((rows, width), F32),
            pltpu.VMEM((mpad, width), F32),
            pltpu.VMEM((2, 8, width), F32),
            pltpu.VMEM((width, width), BF16),
            pltpu.VMEM((width, width), BF16),
            pltpu.VMEM((4, inbox, width // 2), BF16),
            pltpu.VMEM((rows, width), BF16),
            pltpu.VMEM((rows, width), BF16),
            pltpu.VMEM((n + 1, 2, width), F32),
            pltpu.VMEM((n, 2, width), F32),
            pltpu.VMEM((2, mrows, width), F32),
            pltpu.VMEM((2, mrows, width), F32),
            pltpu.VMEM((everyone, mrows, width), BF16),
            pltpu.VMEM((everyone, mrows, width), BF16),
            dma((2, 2)),
            dma((2, 2)),
            dma((4, n, 2)),
            dma((4, n, 2)),
            dma((2, n, 2)),
            dma((n, 2)),
            dma((n, 2)),
        ],
        compiler_params=pltpu.CompilerParams(collective_id=0, has_side_effects=True),
        name="edge_backward",
    )(
        grid_latent,
        mesh_latent[0],
        grid_output_cotangent,
        w_send,
        w_recv,
        output_weight,
        hidden_layer_bias[None],
        output_norm_gain[None],
        edge_sender,
        edge_receiver,
        edge_live,
    )
    return (
        d_grid,
        d_mesh[None],
        d_w_send,
        d_w_recv,
        d_w_out,
        d_vec[0],
        d_vec[1],
    )


def solution(mesh):
    return jax.shard_map(
        body,
        mesh=mesh,
        in_specs=(
            P("space", None),
            P("level", "space", None),
            P("space", None),
            P(),
            P(),
            P(),
            P(),
            P(),
            P("level", "space"),
            P("level", "space"),
            P("level", "space"),
        ),
        out_specs=(P(("space", "level"), None), P("level", "space", None), P(), P(), P(), P(), P()),
        check_vma=False,
    )
```

```python
import functools

import jax
import jax.numpy as jnp
from jax import lax
from jax.experimental import pallas as pl
from jax.experimental.pallas import tpu as pltpu
from jax.sharding import PartitionSpec as P

MESH = pl.DeviceIdType.MESH
F32 = jnp.float32
BF16 = jnp.bfloat16
TILE = 16


def mm(a, b, ca=1, cb=0):
    return lax.dot_general(a, b, (((ca,), (cb,)), ((), ())), preferred_element_type=F32)


def bit_steps(axis, count):
    steps = []
    width = 1
    while width < count:
        steps.append((axis, width))
        width *= 2
    return steps


def exchange_groups(n_space, n_level):
    bits = bit_steps("level", n_level) + bit_steps("space", n_space)
    return [bits[:1]] + [bits[k : k + 2] for k in range(1, len(bits), 2)]


def members(group):
    bits = [(lax.axis_index(axis) // w) % 2 for axis, w in group]
    mine = sum(bit << j for j, bit in enumerate(bits))
    others = []
    for mask in range(1, 1 << len(group)):
        place, who = 0, {}
        for j, (axis, w) in enumerate(group):
            flip = (mask >> j) & 1
            place = place + ((1 - bits[j]) if flip else bits[j]) * (1 << j)
            if flip:
                who[axis] = who.get(axis, lax.axis_index(axis)) + (1 - 2 * bits[j]) * w
        others.append((place, who))
    return mine, others


def reversed_chunks(count):
    order = [0]
    width = 1
    while width < count:
        order = [2 * c for c in order] + [2 * c + 1 for c in order]
        width *= 2
    return order


def pieces(rows, groups):
    plan = []
    size = rows
    for group in groups:
        m = 1 << len(group)
        split = (size // m) % TILE == 0
        size = size // m if split else size
        plan.append((group, size, split))
    return plan


def inbox_rows(rows, groups):
    return sum(((1 << len(group)) - 1) * size for group, size, _ in pieces(rows, groups))


def remote(src, dst, sem, who):
    return pltpu.make_async_remote_copy(
        src_ref=src,
        dst_ref=dst,
        send_sem=sem.at[0],
        recv_sem=sem.at[1],
        device_id=who,
        device_id_type=MESH,
    )


def start_all(copies):
    for c in copies:
        c.start()


def wait_all(copies):
    for c in copies:
        c.wait()


def reduce_lane(buf, out, inbox, sem_r, sem_g, groups):
    off = 0
    spot = 0
    trail = []
    for k, (group, size, split) in enumerate(pieces(buf.shape[0], groups)):
        mine, others = members(group)
        copies, slots = [], []
        for j, (place, who) in enumerate(others):
            give = pl.ds(pl.multiple_of(off + place * size if split else off, TILE), size)
            slot = pl.ds(spot, size)
            copies.append(remote(buf.at[give], inbox.at[slot], sem_r.at[k, j], who))
            slots.append(slot)
            spot += size
        start_all(copies)
        yield
        wait_all(copies)
        off = off + mine * size if split else off
        keep = pl.ds(pl.multiple_of(off, TILE), size)
        total = buf[keep].astype(F32)
        for slot in slots:
            total = total + inbox[slot].astype(F32)
        buf[keep] = total.astype(BF16)
        if split:
            trail.append((k, mine, others, size))
    at = pl.ds(pl.multiple_of(off, TILE), trail[-1][3])
    out[at] = buf[at]
    for k, mine, others, size in reversed(trail):
        at = pl.ds(pl.multiple_of(off, TILE), size)
        copies = [remote(out.at[at], out.at[at], sem_g.at[k, j], who) for j, (_, who) in enumerate(others)]
        start_all(copies)
        yield
        wait_all(copies)
        off = off - mine * size


def gather_lane(buf, sem, groups):
    base = gather_place(groups)
    held = 1
    for k, group in enumerate(reversed(groups)):
        mine, others = members(group)
        at = pl.ds(base, held)
        copies = [remote(buf.at[at], buf.at[at], sem.at[k, j], who) for j, (_, who) in enumerate(others)]
        start_all(copies)
        yield
        wait_all(copies)
        base = base - mine * held
        held <<= len(group)


def gather_place(groups):
    place = 0
    held = 1
    for group in reversed(groups):
        place = place + members(group)[0] * held
        held <<= len(group)
    return place


def grid_lane(gbuf, inbox, dgrid_ref, wrecv_ref, sem, n_level):
    off = 0
    size = gbuf.shape[0]
    spot = 0
    for k, (axis, w) in enumerate(bit_steps("level", n_level)):
        bit, [(_, who)] = members([(axis, w)])
        size //= 2
        give = pl.ds(pl.multiple_of(off + (1 - bit) * size, TILE), size)
        keep = pl.ds(pl.multiple_of(off + bit * size, TILE), size)
        into = pl.ds(spot, size)
        c = remote(gbuf.at[give], inbox.at[into], sem.at[k], who)
        c.start()
        yield
        c.wait()
        gbuf[keep] = (gbuf[keep].astype(F32) + inbox[into].astype(F32)).astype(BF16)
        spot += size
        off = off + bit * size
    dgrid_ref[...] = mm(gbuf[pl.ds(pl.multiple_of(off, TILE), size)], wrecv_ref[...], 1, 1)


def vec_lane(vec, inbox, dvec_ref, sem, groups):
    for k, group in enumerate(groups):
        _, others = members(group)
        copies = [
            remote(vec.at[k], inbox.at[k, j], sem.at[k, j], who) for j, (_, who) in enumerate(others)
        ]
        start_all(copies)
        yield
        wait_all(copies)
        if len(others) == 3:
            vec[k + 1] = (vec[k] + inbox[k, 0]) + (inbox[k, 1] + inbox[k, 2])
        else:
            vec[k + 1] = vec[k] + inbox[k, 0]
    dvec_ref[...] = vec[len(groups)]


def edge_copies(up, down):
    n_space = lax.axis_size("space")
    band = lax.axis_index("space")
    first = band > 0
    last = band < n_space - 1

    def start():
        @pl.when(last)
        def _():
            up.start()

        @pl.when(first)
        def _():
            down.start()

    def wait():
        @pl.when(last)
        def _():
            up.wait_send()
            down.wait_recv()

        @pl.when(first)
        def _():
            down.wait_send()
            up.wait_recv()

    return start, wait


def advance(lanes):
    for lane in list(lanes):
        if next(lane, "end") == "end":
            lanes.remove(lane)


def kernel(
    n_space,
    n_level,
    block,
    segments,
    grid_ref,
    mesh_ref,
    cot_ref,
    wsend_ref,
    wrecv_ref,
    wout_ref,
    bias_ref,
    gain_ref,
    snd_ref,
    rcv_ref,
    live_ref,
    dgrid_ref,
    dmesh_ref,
    dwo_ref,
    dwr_ref,
    dws_ref,
    dvec_ref,
    window,
    table,
    proj,
    pre,
    ups,
    dout,
    wacc,
    gacc,
    macc,
    vacc,
    red_o,
    red_r,
    inbox,
    gbuf,
    gbuf_in,
    vec,
    vec_in,
    mout,
    m_in,
    mesh_all,
    sum_all,
    halo_sem,
    mgrad_sem,
    red_sem,
    gat_sem,
    mesh_sem,
    grid_sem,
    vec_sem,
):
    rows, width = grid_ref.shape
    mrows = mesh_ref.shape[0]
    slots = snd_ref.shape[1]
    band = lax.axis_index("space")
    groups = exchange_groups(n_space, n_level)
    pad = table.shape[0]

    window[...] = jnp.zeros_like(window)
    m_in[...] = jnp.zeros_like(m_in)
    barrier = pltpu.get_barrier_semaphore()
    peers = [who for group in groups for _, who in members(group)[1]]
    for who in peers:
        pl.semaphore_signal(barrier, inc=1, device_id=who, device_id_type=MESH)
    up = {"space": (band + 1) % n_space}
    down = {"space": (band + n_space - 1) % n_space}
    pl.semaphore_signal(barrier, inc=1, device_id=up, device_id_type=MESH)
    pl.semaphore_signal(barrier, inc=1, device_id=down, device_id_type=MESH)
    macc[...] = jnp.zeros_like(macc)
    wacc[...] = jnp.zeros_like(wacc)
    gacc[...] = jnp.zeros_like(gacc)
    vacc[...] = jnp.zeros_like(vacc)
    window[1] = mesh_ref[...]
    place = gather_place(groups)
    mesh_all[place] = mesh_ref[...]
    proj[...] = mm(grid_ref[...], wrecv_ref[...]).astype(BF16)
    pl.semaphore_wait(barrier, len(peers) + 2)

    halo_start, halo_wait = edge_copies(
        remote(mesh_ref, window.at[0], halo_sem.at[0], up),
        remote(mesh_ref, window.at[2], halo_sem.at[1], down),
    )
    halo_start()
    early = [gather_lane(mesh_all, mesh_sem.at[0], groups)]
    advance(early)

    def span(i):
        return pl.ds(pl.multiple_of(i * block, block), block)

    def column(v):
        return jnp.transpose(jnp.broadcast_to(v, (128, block)))

    def one_hot(hit):
        return hit.astype(F32).astype(BF16)

    def source(at):
        snd = snd_ref[:, at]
        slot = snd // mrows
        target = band + slot - 1
        slot = jnp.where((target >= 0) & (target < n_space), slot, 1)
        return slot * mrows + snd % mrows

    def gathers(i, _):
        at = span(i)
        rcv_c = column(rcv_ref[:, at])
        live_c = column(live_ref[:, at].astype(F32))
        pick = one_hot(
            jnp.concatenate([rcv_c] * (rows // 128), axis=1)
            == lax.broadcasted_iota(jnp.int32, (block, rows), 1)
        )
        pre[at] = mm(pick, proj[...]) + bias_ref[...]
        ups[at] = (mm(pick, cot_ref[...]) * jnp.concatenate([live_c] * (width // 128), axis=1)).astype(BF16)
        return 0

    count = slots // block
    lax.fori_loop(0, count, gathers, 0)

    halo_wait()
    win = jnp.concatenate(
        [window[k].astype(F32) for k in range(3)] + [jnp.zeros((pad - 3 * mrows, width), F32)], axis=0
    ).astype(BF16)
    table[...] = mm(win, wsend_ref[...]).astype(BF16)

    def forward(i, _):
        at = span(i)
        src_c = column(source(at))
        pick = one_hot(
            jnp.concatenate([src_c] * (pad // 128), axis=1)
            == lax.broadcasted_iota(jnp.int32, (block, pad), 1)
        )
        preact = pre[at] + mm(pick, table[...])
        sig = jax.nn.sigmoid(preact)
        hidden = (preact * sig).astype(BF16)
        pre[at] = sig * (1.0 + preact * (1.0 - sig))
        outer = mm(hidden, wout_ref[...])
        center = outer - jnp.mean(outer, axis=-1, keepdims=True)
        inv = lax.rsqrt(jnp.mean(center * center, axis=-1, keepdims=True) + 1e-05)
        normed = center * inv
        upstream = ups[at].astype(F32)
        scaled = upstream * gain_ref[...]
        d_outer = inv * (
            scaled
            - jnp.mean(scaled, axis=-1, keepdims=True)
            - normed * jnp.mean(scaled * normed, axis=-1, keepdims=True)
        )
        d_outer = d_outer.astype(BF16)
        dout[at] = d_outer
        wacc[...] += mm(hidden, d_outer, 0, 0)
        vacc[1] += jnp.sum((upstream * normed).reshape(block // 8, 8, width), axis=0)
        return 0

    def backward(i, _):
        at = span(i)
        put = one_hot(
            jnp.broadcast_to(rcv_ref[:, at], (rows, block))
            == lax.broadcasted_iota(jnp.int32, (rows, block), 0)
        )
        put_s = one_hot(
            jnp.broadcast_to(source(at), (macc.shape[0], block))
            == lax.broadcasted_iota(jnp.int32, (macc.shape[0], block), 0)
        )
        d_pre = mm(dout[at], wout_ref[...], 1, 1) * pre[at]
        vacc[0] += jnp.sum(d_pre.reshape(block // 8, 8, width), axis=0)
        d_pre = d_pre.astype(BF16)
        gacc[...] += mm(put, d_pre)
        macc[...] += mm(put_s, d_pre)
        return 0

    cuts = [count * k // segments for k in range(segments + 1)]
    for lo, hi in zip(cuts, cuts[1:]):
        lax.fori_loop(lo, hi, forward, 0)
        advance(early)

    def reducer(buf, out, k):
        return reduce_lane(buf, out, inbox.at[k], red_sem.at[k], gat_sem.at[k], groups)

    red_o[...] = wacc[...].astype(BF16)
    out_lanes = [reducer(red_o, dwo_ref, 0)] + early
    advance(out_lanes)
    for lo, hi in zip(cuts, cuts[1:]):
        lax.fori_loop(lo, hi, backward, 0)
        if hi < count:
            advance(out_lanes)

    red_r[...] = mm(grid_ref[...], gacc[...].astype(BF16), 0, 0).astype(BF16)
    lanes = [reducer(red_r, dwr_ref, 1)]
    advance(lanes)

    def mesh_lane():
        mout[0] = macc[0:mrows]
        mout[1] = macc[2 * mrows : 3 * mrows]
        start, wait = edge_copies(
            remote(mout.at[1], m_in.at[0], mgrad_sem.at[0], up),
            remote(mout.at[0], m_in.at[1], mgrad_sem.at[1], down),
        )
        start()
        yield
        wait()
        total = macc[mrows : 2 * mrows] + m_in[0] + m_in[1]
        sum_all[place] = total.astype(BF16)
        lane = gather_lane(sum_all, mesh_sem.at[1], groups)
        next(lane)
        total = jnp.concatenate([total, jnp.zeros((TILE - mrows % TILE, width), F32)], axis=0)
        dmesh_ref[...] = mm(total.astype(BF16), wsend_ref[...], 1, 1)[0:mrows]
        yield
        yield from lane
        every = mesh_all.shape[0] * mrows
        dws_ref[...] = mm(
            mesh_all[...].astype(F32).reshape(every, width).astype(BF16),
            sum_all[...].astype(F32).reshape(every, width).astype(BF16),
            0,
            0,
        ).astype(BF16)

    share = rows // n_level
    for spot, chunk in enumerate(reversed_chunks(n_level)):
        gbuf[spot * share : (spot + 1) * share] = gacc[chunk * share : (chunk + 1) * share].astype(BF16)
    vec[0] = jnp.concatenate([jnp.sum(vacc[k], axis=0, keepdims=True) for k in range(2)], axis=0)
    small = [
        mesh_lane(),
        grid_lane(gbuf, gbuf_in, dgrid_ref, wrecv_ref, grid_sem, n_level),
        vec_lane(vec, vec_in, dvec_ref, vec_sem, groups),
    ]
    advance(small)
    lanes = lanes + small + out_lanes
    while lanes:
        advance(lanes)


def body(
    grid_latent,
    mesh_latent,
    grid_output_cotangent,
    w_send,
    w_recv,
    output_weight,
    hidden_layer_bias,
    output_norm_gain,
    edge_sender,
    edge_receiver,
    edge_live,
):
    n_space = lax.axis_size("space")
    n_level = lax.axis_size("level")
    rows, width = grid_latent.shape
    mrows = mesh_latent.shape[1]
    slots = edge_sender.shape[1]
    block = min(256, slots)
    pad = -(-3 * mrows // 128) * 128
    mpad = -(-3 * mrows // TILE) * TILE
    groups = exchange_groups(n_space, n_level)
    n = len(groups)
    inbox = inbox_rows(width, groups)
    vm = pl.BlockSpec(memory_space=pltpu.VMEM)
    dma = pltpu.SemaphoreType.DMA
    everyone = n_space * n_level
    d_grid, d_mesh, d_w_out, d_w_recv, d_w_send, d_vec = pl.pallas_call(
        functools.partial(kernel, n_space, n_level, block, min(4, slots // block)),
        out_shape=(
            jax.ShapeDtypeStruct((rows // n_level, width), F32),
            jax.ShapeDtypeStruct((mrows, width), F32),
            jax.ShapeDtypeStruct((width, width), BF16),
            jax.ShapeDtypeStruct((width, width), BF16),
            jax.ShapeDtypeStruct((width, width), BF16),
            jax.ShapeDtypeStruct((2, width), F32),
        ),
        in_specs=[vm] * 11,
        out_specs=(vm,) * 6,
        scratch_shapes=[
            pltpu.VMEM((3, mrows, width), BF16),
            pltpu.VMEM((pad, width), BF16),
            pltpu.VMEM((rows, width), BF16),
            pltpu.VMEM((slots, width), F32),
            pltpu.VMEM((slots, width), BF16),
            pltpu.VMEM((slots, width), BF16),
            pltpu.VMEM((width, width), F32),
            pltpu.VMEM((rows, width), F32),
            pltpu.VMEM((mpad, width), F32),
            pltpu.VMEM((2, 8, width), F32),
            pltpu.VMEM((width, width), BF16),
            pltpu.VMEM((width, width), BF16),
            pltpu.VMEM((2, inbox, width), BF16),
            pltpu.VMEM((rows, width), BF16),
            pltpu.VMEM((rows, width), BF16),
            pltpu.VMEM((n + 1, 2, width), F32),
            pltpu.VMEM((n, 3, 2, width), F32),
            pltpu.VMEM((2, mrows, width), F32),
            pltpu.VMEM((2, mrows, width), F32),
            pltpu.VMEM((everyone, mrows, width), BF16),
            pltpu.VMEM((everyone, mrows, width), BF16),
            dma((2, 2)),
            dma((2, 2)),
            dma((2, n, 3, 2)),
            dma((2, n, 3, 2)),
            dma((2, n, 3, 2)),
            dma((len(bit_steps("level", n_level)), 2)),
            dma((n, 3, 2)),
        ],
        compiler_params=pltpu.CompilerParams(collective_id=0, has_side_effects=True),
        name="edge_backward",
    )(
        grid_latent,
        mesh_latent[0],
        grid_output_cotangent,
        w_send,
        w_recv,
        output_weight,
        hidden_layer_bias[None],
        output_norm_gain[None],
        edge_sender,
        edge_receiver,
        edge_live,
    )
    return (
        d_grid,
        d_mesh[None],
        d_w_send,
        d_w_recv,
        d_w_out,
        d_vec[0],
        d_vec[1],
    )


def solution(mesh):
    return jax.shard_map(
        body,
        mesh=mesh,
        in_specs=(
            P("space", None),
            P("level", "space", None),
            P("space", None),
            P(),
            P(),
            P(),
            P(),
            P(),
            P("level", "space"),
            P("level", "space"),
            P("level", "space"),
        ),
        out_specs=(P(("space", "level"), None), P("level", "space", None), P(), P(), P(), P(), P()),
        check_vma=False,
    )
```

```python
import functools

import jax
import jax.numpy as jnp
from jax import lax
from jax.experimental import pallas as pl
from jax.experimental.pallas import tpu as pltpu
from jax.sharding import PartitionSpec as P

MESH = pl.DeviceIdType.MESH
F32 = jnp.float32
BF16 = jnp.bfloat16
TILE = 16


def mm(a, b, ca=1, cb=0):
    return lax.dot_general(a, b, (((ca,), (cb,)), ((), ())), preferred_element_type=F32)


def bit_steps(axis, count):
    steps = []
    width = 1
    while width < count:
        steps.append((axis, width))
        width *= 2
    return steps


def exchange_groups(n_space, n_level):
    bits = bit_steps("level", n_level) + bit_steps("space", n_space)
    return [bits[:1]] + [bits[k : k + 2] for k in range(1, len(bits), 2)]


def members(group):
    bits = [(lax.axis_index(axis) // w) % 2 for axis, w in group]
    mine = sum(bit << j for j, bit in enumerate(bits))
    others = []
    for mask in range(1, 1 << len(group)):
        place, who = 0, {}
        for j, (axis, w) in enumerate(group):
            flip = (mask >> j) & 1
            place = place + ((1 - bits[j]) if flip else bits[j]) * (1 << j)
            if flip:
                who[axis] = who.get(axis, lax.axis_index(axis)) + (1 - 2 * bits[j]) * w
        others.append((place, who))
    return mine, others


def reversed_chunks(count):
    order = [0]
    width = 1
    while width < count:
        order = [2 * c for c in order] + [2 * c + 1 for c in order]
        width *= 2
    return order


def pieces(rows, groups):
    plan = []
    size = rows
    for group in groups:
        m = 1 << len(group)
        split = (size // m) % TILE == 0
        size = size // m if split else size
        plan.append((group, size, split))
    return plan


def inbox_rows(rows, groups):
    return sum(((1 << len(group)) - 1) * size for group, size, _ in pieces(rows, groups))


def remote(src, dst, sem, who):
    return pltpu.make_async_remote_copy(
        src_ref=src,
        dst_ref=dst,
        send_sem=sem.at[0],
        recv_sem=sem.at[1],
        device_id=who,
        device_id_type=MESH,
    )


def start_all(copies):
    for c in copies:
        c.start()


def wait_all(copies):
    for c in copies:
        c.wait()


def reduce_lane(buf, out, inbox, sem_r, sem_g, groups):
    off = 0
    spot = 0
    trail = []
    for k, (group, size, split) in enumerate(pieces(buf.shape[0], groups)):
        mine, others = members(group)
        copies, slots = [], []
        for j, (place, who) in enumerate(others):
            give = pl.ds(pl.multiple_of(off + place * size if split else off, TILE), size)
            slot = pl.ds(spot, size)
            copies.append(remote(buf.at[give], inbox.at[slot], sem_r.at[k, j], who))
            slots.append(slot)
            spot += size
        start_all(copies)
        yield
        wait_all(copies)
        off = off + mine * size if split else off
        keep = pl.ds(pl.multiple_of(off, TILE), size)
        total = buf[keep].astype(F32)
        for slot in slots:
            total = total + inbox[slot].astype(F32)
        buf[keep] = total.astype(BF16)
        if split:
            trail.append((k, mine, others, size))
    at = pl.ds(pl.multiple_of(off, TILE), trail[-1][3])
    out[at] = buf[at]
    for k, mine, others, size in reversed(trail):
        at = pl.ds(pl.multiple_of(off, TILE), size)
        copies = [remote(out.at[at], out.at[at], sem_g.at[k, j], who) for j, (_, who) in enumerate(others)]
        start_all(copies)
        yield
        wait_all(copies)
        off = off - mine * size


def gather_lane(buf, sem, groups):
    base = gather_place(groups)
    held = 1
    for k, group in enumerate(reversed(groups)):
        mine, others = members(group)
        at = pl.ds(base, held)
        copies = [remote(buf.at[at], buf.at[at], sem.at[k, j], who) for j, (_, who) in enumerate(others)]
        start_all(copies)
        yield
        wait_all(copies)
        base = base - mine * held
        held <<= len(group)


def gather_place(groups):
    place = 0
    held = 1
    for group in reversed(groups):
        place = place + members(group)[0] * held
        held <<= len(group)
    return place


def grid_lane(gbuf, inbox, dgrid_ref, wrecv_ref, sem, n_level):
    off = 0
    size = gbuf.shape[0]
    spot = 0
    for k, (axis, w) in enumerate(bit_steps("level", n_level)):
        bit, [(_, who)] = members([(axis, w)])
        size //= 2
        give = pl.ds(pl.multiple_of(off + (1 - bit) * size, TILE), size)
        keep = pl.ds(pl.multiple_of(off + bit * size, TILE), size)
        into = pl.ds(spot, size)
        c = remote(gbuf.at[give], inbox.at[into], sem.at[k], who)
        c.start()
        yield
        c.wait()
        gbuf[keep] = (gbuf[keep].astype(F32) + inbox[into].astype(F32)).astype(BF16)
        spot += size
        off = off + bit * size
    dgrid_ref[...] = mm(gbuf[pl.ds(pl.multiple_of(off, TILE), size)], wrecv_ref[...], 1, 1)


def vec_lane(vec, inbox, dvec_ref, sem, groups):
    for k, group in enumerate(groups):
        _, others = members(group)
        copies = [
            remote(vec.at[k], inbox.at[k, j], sem.at[k, j], who) for j, (_, who) in enumerate(others)
        ]
        start_all(copies)
        yield
        wait_all(copies)
        if len(others) == 3:
            vec[k + 1] = (vec[k] + inbox[k, 0]) + (inbox[k, 1] + inbox[k, 2])
        else:
            vec[k + 1] = vec[k] + inbox[k, 0]
    dvec_ref[...] = vec[len(groups)]


def edge_copies(up, down):
    n_space = lax.axis_size("space")
    band = lax.axis_index("space")
    first = band > 0
    last = band < n_space - 1

    def start():
        @pl.when(last)
        def _():
            up.start()

        @pl.when(first)
        def _():
            down.start()

    def wait():
        @pl.when(last)
        def _():
            up.wait_send()
            down.wait_recv()

        @pl.when(first)
        def _():
            down.wait_send()
            up.wait_recv()

    return start, wait


def advance(lanes):
    for lane in list(lanes):
        if next(lane, "end") == "end":
            lanes.remove(lane)


def kernel(
    n_space,
    n_level,
    block,
    segments,
    grid_ref,
    mesh_ref,
    cot_ref,
    wsend_ref,
    wrecv_ref,
    wout_ref,
    bias_ref,
    gain_ref,
    snd_ref,
    rcv_ref,
    live_ref,
    dgrid_ref,
    dmesh_ref,
    dwo_ref,
    dwr_ref,
    dws_ref,
    dvec_ref,
    window,
    table,
    proj,
    pre,
    ups,
    dout,
    wacc,
    gacc,
    macc,
    vacc,
    red_o,
    red_r,
    inbox,
    gbuf,
    gbuf_in,
    vec,
    vec_in,
    mout,
    m_in,
    mesh_all,
    sum_all,
    halo_sem,
    mgrad_sem,
    red_sem,
    gat_sem,
    mesh_sem,
    grid_sem,
    vec_sem,
):
    rows, width = grid_ref.shape
    mrows = mesh_ref.shape[0]
    slots = snd_ref.shape[1]
    band = lax.axis_index("space")
    groups = exchange_groups(n_space, n_level)
    pad = table.shape[0]

    window[...] = jnp.zeros_like(window)
    m_in[...] = jnp.zeros_like(m_in)
    barrier = pltpu.get_barrier_semaphore()
    peers = [who for group in groups for _, who in members(group)[1]]
    for who in peers:
        pl.semaphore_signal(barrier, inc=1, device_id=who, device_id_type=MESH)
    up = {"space": (band + 1) % n_space}
    down = {"space": (band + n_space - 1) % n_space}
    pl.semaphore_signal(barrier, inc=1, device_id=up, device_id_type=MESH)
    pl.semaphore_signal(barrier, inc=1, device_id=down, device_id_type=MESH)
    macc[...] = jnp.zeros_like(macc)
    wacc[...] = jnp.zeros_like(wacc)
    gacc[...] = jnp.zeros_like(gacc)
    vacc[...] = jnp.zeros_like(vacc)
    window[1] = mesh_ref[...]
    place = gather_place(groups)
    mesh_all[place] = mesh_ref[...]
    proj[...] = mm(grid_ref[...], wrecv_ref[...]).astype(BF16)
    pl.semaphore_wait(barrier, len(peers) + 2)

    halo_start, halo_wait = edge_copies(
        remote(mesh_ref, window.at[0], halo_sem.at[0], up),
        remote(mesh_ref, window.at[2], halo_sem.at[1], down),
    )
    halo_start()
    early = [gather_lane(mesh_all, mesh_sem.at[0], groups)]
    advance(early)

    def span(i):
        return pl.ds(pl.multiple_of(i * block, block), block)

    def column(v):
        return jnp.transpose(jnp.broadcast_to(v, (128, block)))

    def one_hot(hit):
        return hit.astype(F32).astype(BF16)

    def source(at):
        snd = snd_ref[:, at]
        slot = snd // mrows
        target = band + slot - 1
        slot = jnp.where((target >= 0) & (target < n_space), slot, 1)
        return slot * mrows + snd % mrows

    def gathers(i, _):
        at = span(i)
        rcv_c = column(rcv_ref[:, at])
        live_c = column(live_ref[:, at].astype(F32))
        pick = one_hot(
            jnp.concatenate([rcv_c] * (rows // 128), axis=1)
            == lax.broadcasted_iota(jnp.int32, (block, rows), 1)
        )
        pre[at] = mm(pick, proj[...]) + bias_ref[...]
        ups[at] = (mm(pick, cot_ref[...]) * jnp.concatenate([live_c] * (width // 128), axis=1)).astype(BF16)
        return 0

    count = slots // block
    lax.fori_loop(0, count, gathers, 0)

    halo_wait()
    win = jnp.concatenate(
        [window[k].astype(F32) for k in range(3)] + [jnp.zeros((pad - 3 * mrows, width), F32)], axis=0
    ).astype(BF16)
    table[...] = mm(win, wsend_ref[...]).astype(BF16)

    def forward(i, _):
        at = span(i)
        src_c = column(source(at))
        pick = one_hot(
            jnp.concatenate([src_c] * (pad // 128), axis=1)
            == lax.broadcasted_iota(jnp.int32, (block, pad), 1)
        )
        preact = pre[at] + mm(pick, table[...])
        sig = jax.nn.sigmoid(preact)
        hidden = (preact * sig).astype(BF16)
        pre[at] = sig * (1.0 + preact * (1.0 - sig))
        outer = mm(hidden, wout_ref[...])
        center = outer - jnp.mean(outer, axis=-1, keepdims=True)
        inv = lax.rsqrt(jnp.mean(center * center, axis=-1, keepdims=True) + 1e-05)
        normed = center * inv
        upstream = ups[at].astype(F32)
        scaled = upstream * gain_ref[...]
        d_outer = inv * (
            scaled
            - jnp.mean(scaled, axis=-1, keepdims=True)
            - normed * jnp.mean(scaled * normed, axis=-1, keepdims=True)
        )
        d_outer = d_outer.astype(BF16)
        dout[at] = d_outer
        wacc[...] += mm(hidden, d_outer, 0, 0)
        vacc[1] += jnp.sum((upstream * normed).reshape(block // 8, 8, width), axis=0)
        return 0

    def backward(i, _):
        at = span(i)
        put = one_hot(
            jnp.broadcast_to(rcv_ref[:, at], (rows, block))
            == lax.broadcasted_iota(jnp.int32, (rows, block), 0)
        )
        put_s = one_hot(
            jnp.broadcast_to(source(at), (macc.shape[0], block))
            == lax.broadcasted_iota(jnp.int32, (macc.shape[0], block), 0)
        )
        d_pre = mm(dout[at], wout_ref[...], 1, 1) * pre[at]
        vacc[0] += jnp.sum(d_pre.reshape(block // 8, 8, width), axis=0)
        d_pre = d_pre.astype(BF16)
        gacc[...] += mm(put, d_pre)
        macc[...] += mm(put_s, d_pre)
        return 0

    cuts = [count * k // segments for k in range(segments + 1)]
    for lo, hi in zip(cuts, cuts[1:]):
        lax.fori_loop(lo, hi, forward, 0)
        advance(early)

    def reducer(buf, out, k):
        return reduce_lane(buf, out, inbox.at[k], red_sem.at[k], gat_sem.at[k], groups)

    red_o[...] = wacc[...].astype(BF16)
    out_lanes = [reducer(red_o, dwo_ref, 0)] + early
    advance(out_lanes)
    for lo, hi in zip(cuts, cuts[1:]):
        lax.fori_loop(lo, hi, backward, 0)
        if hi < count:
            advance(out_lanes)

    red_r[...] = mm(grid_ref[...], gacc[...].astype(BF16), 0, 0).astype(BF16)
    lanes = [reducer(red_r, dwr_ref, 1)]
    advance(lanes)

    def mesh_lane():
        mout[0] = macc[0:mrows]
        mout[1] = macc[2 * mrows : 3 * mrows]
        start, wait = edge_copies(
            remote(mout.at[1], m_in.at[0], mgrad_sem.at[0], up),
            remote(mout.at[0], m_in.at[1], mgrad_sem.at[1], down),
        )
        start()
        yield
        wait()
        total = macc[mrows : 2 * mrows] + m_in[0] + m_in[1]
        sum_all[place] = total.astype(BF16)
        lane = gather_lane(sum_all, mesh_sem.at[1], groups)
        next(lane)
        total = jnp.concatenate([total, jnp.zeros((TILE - mrows % TILE, width), F32)], axis=0)
        dmesh_ref[...] = mm(total.astype(BF16), wsend_ref[...], 1, 1)[0:mrows]
        yield
        yield from lane
        every = mesh_all.shape[0] * mrows
        dws_ref[...] = mm(
            mesh_all[...].astype(F32).reshape(every, width).astype(BF16),
            sum_all[...].astype(F32).reshape(every, width).astype(BF16),
            0,
            0,
        ).astype(BF16)

    share = rows // n_level
    for spot, chunk in enumerate(reversed_chunks(n_level)):
        gbuf[spot * share : (spot + 1) * share] = gacc[chunk * share : (chunk + 1) * share].astype(BF16)
    vec[0] = jnp.concatenate([jnp.sum(vacc[k], axis=0, keepdims=True) for k in range(2)], axis=0)
    small = [
        mesh_lane(),
        grid_lane(gbuf, gbuf_in, dgrid_ref, wrecv_ref, grid_sem, n_level),
        vec_lane(vec, vec_in, dvec_ref, vec_sem, groups),
    ]
    advance(small)
    lanes = lanes + small + out_lanes
    while lanes:
        advance(lanes)


def hand_out(
    grid_in,
    mesh_in,
    wo_in,
    wr_in,
    ws_in,
    vec_in,
    grid_out,
    mesh_out,
    wo_out,
    wr_out,
    ws_out,
    bias_out,
    gain_out,
    grid_mid,
    mesh_mid,
    wo_mid,
    wr_mid,
    ws_mid,
    sem,
):
    trips = [
        (grid_in, grid_mid, grid_out),
        (mesh_in, mesh_mid, mesh_out.at[0]),
        (wo_in, wo_mid, wo_out),
        (wr_in, wr_mid, wr_out),
        (ws_in, ws_mid, ws_out),
    ]
    loads = [pltpu.make_async_copy(a, b, sem.at[0, k]) for k, (a, b, _) in enumerate(trips)]
    stores = [pltpu.make_async_copy(b, c, sem.at[1, k]) for k, (_, b, c) in enumerate(trips)]
    start_all(loads)
    bias_out[...] = vec_in[0]
    gain_out[...] = vec_in[1]
    for load, store in zip(loads, stores):
        load.wait()
        store.start()
    wait_all(stores)


def body(
    grid_latent,
    mesh_latent,
    grid_output_cotangent,
    w_send,
    w_recv,
    output_weight,
    hidden_layer_bias,
    output_norm_gain,
    edge_sender,
    edge_receiver,
    edge_live,
):
    n_space = lax.axis_size("space")
    n_level = lax.axis_size("level")
    rows, width = grid_latent.shape
    mrows = mesh_latent.shape[1]
    slots = edge_sender.shape[1]
    block = min(512, slots)
    pad = -(-3 * mrows // 128) * 128
    mpad = -(-3 * mrows // TILE) * TILE
    groups = exchange_groups(n_space, n_level)
    n = len(groups)
    inbox = inbox_rows(width, groups)
    vm = pl.BlockSpec(memory_space=pltpu.VMEM)
    dma = pltpu.SemaphoreType.DMA
    everyone = n_space * n_level
    d_grid, d_mesh, d_w_out, d_w_recv, d_w_send, d_vec = pl.pallas_call(
        functools.partial(kernel, n_space, n_level, block, min(4, slots // block)),
        out_shape=(
            jax.ShapeDtypeStruct((rows // n_level, width), F32),
            jax.ShapeDtypeStruct((mrows, width), F32),
            jax.ShapeDtypeStruct((width, width), BF16),
            jax.ShapeDtypeStruct((width, width), BF16),
            jax.ShapeDtypeStruct((width, width), BF16),
            jax.ShapeDtypeStruct((2, width), F32),
        ),
        in_specs=[vm] * 11,
        out_specs=(vm,) * 6,
        scratch_shapes=[
            pltpu.VMEM((3, mrows, width), BF16),
            pltpu.VMEM((pad, width), BF16),
            pltpu.VMEM((rows, width), BF16),
            pltpu.VMEM((slots, width), F32),
            pltpu.VMEM((slots, width), BF16),
            pltpu.VMEM((slots, width), BF16),
            pltpu.VMEM((width, width), F32),
            pltpu.VMEM((rows, width), F32),
            pltpu.VMEM((mpad, width), F32),
            pltpu.VMEM((2, 8, width), F32),
            pltpu.VMEM((width, width), BF16),
            pltpu.VMEM((width, width), BF16),
            pltpu.VMEM((2, inbox, width), BF16),
            pltpu.VMEM((rows, width), BF16),
            pltpu.VMEM((rows, width), BF16),
            pltpu.VMEM((n + 1, 2, width), F32),
            pltpu.VMEM((n, 3, 2, width), F32),
            pltpu.VMEM((2, mrows, width), F32),
            pltpu.VMEM((2, mrows, width), F32),
            pltpu.VMEM((everyone, mrows, width), BF16),
            pltpu.VMEM((everyone, mrows, width), BF16),
            dma((2, 2)),
            dma((2, 2)),
            dma((2, n, 3, 2)),
            dma((2, n, 3, 2)),
            dma((2, n, 3, 2)),
            dma((len(bit_steps("level", n_level)), 2)),
            dma((n, 3, 2)),
        ],
        compiler_params=pltpu.CompilerParams(collective_id=0, has_side_effects=True),
        name="edge_backward",
    )(
        grid_latent,
        mesh_latent[0],
        grid_output_cotangent,
        w_send,
        w_recv,
        output_weight,
        hidden_layer_bias[None],
        output_norm_gain[None],
        edge_sender,
        edge_receiver,
        edge_live,
    )
    hbm = pl.BlockSpec(memory_space=pl.ANY)
    d_grid, d_mesh, d_w_out, d_w_recv, d_w_send, d_bias, d_gain = pl.pallas_call(
        hand_out,
        out_shape=(
            jax.ShapeDtypeStruct(d_grid.shape, F32),
            jax.ShapeDtypeStruct((1,) + d_mesh.shape, F32),
            jax.ShapeDtypeStruct(d_w_out.shape, BF16),
            jax.ShapeDtypeStruct(d_w_recv.shape, BF16),
            jax.ShapeDtypeStruct(d_w_send.shape, BF16),
            jax.ShapeDtypeStruct((width,), F32),
            jax.ShapeDtypeStruct((width,), F32),
        ),
        in_specs=[hbm] * 5 + [vm],
        out_specs=(hbm,) * 5 + (vm,) * 2,
        scratch_shapes=[
            pltpu.VMEM(d_grid.shape, F32),
            pltpu.VMEM(d_mesh.shape, F32),
            pltpu.VMEM(d_w_out.shape, BF16),
            pltpu.VMEM(d_w_recv.shape, BF16),
            pltpu.VMEM(d_w_send.shape, BF16),
            dma((2, 5)),
        ],
        name="hand_out",
    )(d_grid, d_mesh, d_w_out, d_w_recv, d_w_send, d_vec)
    return (d_grid, d_mesh, d_w_send, d_w_recv, d_w_out, d_bias, d_gain)


def solution(mesh):
    return jax.shard_map(
        body,
        mesh=mesh,
        in_specs=(
            P("space", None),
            P("level", "space", None),
            P("space", None),
            P(),
            P(),
            P(),
            P(),
            P(),
            P("level", "space"),
            P("level", "space"),
            P("level", "space"),
        ),
        out_specs=(P(("space", "level"), None), P("level", "space", None), P(), P(), P(), P(), P()),
        check_vma=False,
    )
```
